32 devices in a mesh: tm: 4 (over y, core), space: 8 (over z, x).
Axes of the slice: x: 2, y: 2, z: 4, core: 2. Of those that a mesh axis runs over, the one named last changes fastest.
Arguments:
- state: float32 [4, 4, 16, 128, 128], P('tm', None, 'space'), may hold values from -6 to 6
- source: float32 [4, 4, 16, 128, 128], P('tm', None, 'space'), may hold values from -6 to 6
- start_field: float32 [16, 128, 128], P('space'), may hold values from -6 to 6
- diffusion: float32 [16, 128, 128], P('space'), may hold values from 0.1 to 1
- reaction: float32 [16, 128, 128], P('space'), may hold values from 0.3 to 3
- section_matrix: float32 [4, 4], replicated, may hold values from -0.5 to 3.5, as said below
- end_weights: float32 [4], replicated, may hold values from 0.2 to 0.6
Outputs:
- smoothed: float32 [4, 4, 16, 128, 128], P('tm', None, 'space')
The draws below stay inside these ranges and needn't reach their ends.
Inputs may be any that keep to these rules, and one draw needn't show every extreme that they name: `section_matrix`: diagonal entries lie between 2 and 3.5, the others between -0.5 and 0.5.
All inputs are finite; a program needn't handle non-finite values.
Results may differ from the reference program's by a relative error of at most 0.0001.
Values sent between devices are 32-bit elements; how exact they have to be, the bound alone decides.
No kernel may reach another device: no remote copies, remote signals or barrier semaphores. Data moves between devices by JAX's collectives and lax.ppermute only.
A program may use at most 64 MiB of HBM per device.

```python
import math
import jax
import jax.numpy as jnp
from jax import lax

SECTIONS = 4
NY = 128
NZ = 128
NX = 16
SLABS = 4


def draw_section_matrix(key, part):
    first, second = jax.random.split(jax.random.fold_in(key, 11))
    diag = jax.random.uniform(first, (SECTIONS,), jnp.float32, 2.0, 3.0)
    other = jax.random.uniform(second, (SECTIONS, SECTIONS), jnp.float32, -0.5, 0.5)
    ident = jnp.eye(SECTIONS, dtype=jnp.float32)
    return other * (1.0 - ident) + ident * diag[None, :]


def shard_levels(own_key, shape, cuts, smallest, high):
    factor_of, own = 1.0, jax.random.fold_in(own_key, 6)
    for dim, shards_of in cuts:
        heights = jnp.exp(jax.random.uniform(jax.random.fold_in(own, dim), (shards_of,), jnp.float32, smallest / len(cuts), high / len(cuts)))
        factor_of = factor_of * jnp.repeat(heights, shape[dim] // shards_of).reshape([-1 if axis == dim else 1 for axis in range(len(shape))])
    return factor_of


def bell_draw(own_key, dims, deviation, bound, cuts=(), held_as=jnp.bfloat16):
    drawn = deviation * jax.random.normal(own_key, dims, jnp.float32)
    if cuts:
        drawn = drawn * shard_levels(own_key, dims, cuts, -0.22, 0.18)
    return jnp.clip(drawn, -bound, bound).astype(held_as)


def setup_inputs(seed: int = 0) -> dict:
    streams_of = jax.random.split(jax.random.key(seed), 8)
    return {
        "state": bell_draw(streams_of[0], (SLABS, SECTIONS, NX, NY, NZ), 1.0, 6.0, ((0, 4), (2, 8)), jnp.float32),
        "source": bell_draw(streams_of[1], (SLABS, SECTIONS, NX, NY, NZ), 1.0, 6.0, ((0, 4), (2, 8)), jnp.float32),
        "start_field": bell_draw(streams_of[2], (NX, NY, NZ), 1.0, 6.0, ((0, 8),), jnp.float32),
        "diffusion": jnp.clip(jnp.exp(math.log(1.0) - 2.3025851 * jax.random.uniform(streams_of[3], (NX, NY, NZ), jnp.float32) ** shard_levels(streams_of[3], (NX, NY, NZ), ((0, 8),), -0.2, 0.2)), 0.1, 1.0),
        "reaction": jnp.clip(jnp.exp(math.log(3.0) - 2.3025851 * jax.random.uniform(streams_of[4], (NX, NY, NZ), jnp.float32) ** shard_levels(streams_of[4], (NX, NY, NZ), ((0, 8),), -0.2, 0.2)), 0.3, 3.0),
        "section_matrix": draw_section_matrix(jax.random.fold_in(streams_of[7], 71), 0),
        "end_weights": jnp.clip(jax.random.uniform(streams_of[6], (SECTIONS,), jnp.float32, 0.2, 0.6), 0.2, 0.6),
    }


def laplace(padded):
    center = padded[:, :, 1:-1]
    side = padded[:, :, 2:] + padded[:, :, :-2]
    inner = jnp.pad(center, ((0, 0), (0, 0), (0, 0), (1, 1), (1, 1)))
    side = side + inner[:, :, :, 2:, 1:-1] + inner[:, :, :, :-2, 1:-1]
    side = side + inner[:, :, :, 1:-1, 2:] + inner[:, :, :, 1:-1, :-2]
    return 6.0 * center - side


def section_mix(section_matrix, field):
    return jnp.einsum("sr,nrxyz->nsxyz", section_matrix, field, precision=lax.Precision.HIGHEST)


def end_values(end_weights, field):
    return jnp.einsum("r,nrxyz->nxyz", end_weights, field, precision=lax.Precision.HIGHEST)


def pad_planes(field):
    return jnp.pad(field, ((0, 0), (0, 0), (1, 1), (0, 0), (0, 0)))


def fine_apply(field, section_matrix, end_weights, start_field, diffusion, reaction):
    ends = end_values(end_weights, field)
    before = jnp.concatenate([start_field[None], ends[:-1]], 0)
    return section_mix(section_matrix, field) + diffusion * laplace(pad_planes(field)) + reaction * jnp.tanh(field) - before[:, None]


def coarse_apply(field, section_matrix, end_weights, diffusion, reaction):
    ends = end_values(end_weights, field)
    before = jnp.concatenate([jnp.zeros_like(ends[:1]), ends[:-1]], 0)
    return section_mix(section_matrix, field) + 2.0 * (diffusion * laplace(pad_planes(field)) + reaction * field) - before[:, None]


def reference(state, source, start_field, diffusion, reaction, section_matrix, end_weights):
    diag = jnp.diagonal(section_matrix)[None, :, None, None, None]
    dfine = diag + 6.0 * diffusion + reaction
    dcoarse = diag + 2.0 * (6.0 * diffusion + reaction)
    field = state
    for weight in (0.6, 1.0):
        field = field + weight * (source - fine_apply(field, section_matrix, end_weights, start_field, diffusion, reaction)) / dfine
    res = source - fine_apply(field, section_matrix, end_weights, start_field, diffusion, reaction)
    coarse_res = res[0::2] + res[1::2]
    correction = 0.7 * coarse_res / dcoarse
    for weight in (1.0, 0.7):
        correction = correction + weight * (coarse_res - coarse_apply(correction, section_matrix, end_weights, diffusion, reaction)) / dcoarse
    field = field + jnp.repeat(correction, 2, axis=0)
    for weight in (1.0, 0.6):
        field = field + weight * (source - fine_apply(field, section_matrix, end_weights, start_field, diffusion, reaction)) / dfine
    return field
```

```python
import functools

import jax
import jax.numpy as jnp
from jax import lax
from jax.experimental import pallas as pl
from jax.experimental.pallas import tpu as pltpu
from jax.sharding import PartitionSpec as P

HALO = 8
SUB = 8

VMEM = pl.BlockSpec(memory_space=pltpu.VMEM)
SMEM = pl.BlockSpec(memory_space=pltpu.SMEM)
ANY = pl.BlockSpec(memory_space=pl.ANY)
F32 = jnp.float32


def permutations(slabs, blocks):
    ys, zs = slabs // 2, blocks // 2

    def at(y, c, z, x):
        return (2 * y + c) * blocks + 2 * z + x

    everyone = [(y, c, z, x) for y in range(ys) for c in range(2) for z in range(zs) for x in range(2)]

    def depth(y, c, z, x):
        if c == 1:
            return at(y, 0, z + 1, x) if z + 1 < zs else at(y, 1, z, 1 - x)
        return at(y, 1, z - 1, x) if z > 0 else at(y, 0, z, 1 - x)

    maps = {
        "first": lambda y, c, z, x: at(y, x, z, c),
        "second": lambda y, c, z, x: at(y, x, z, 1 - c),
        "back": lambda y, c, z, x: at(y, 1 - x, z, c),
        "depth": depth,
        "core": lambda y, c, z, x: at(y, 1 - c, z, x),
        "time": lambda y, c, z, x: at((y + 1) % ys, c, z, x),
    }
    return {name: [(at(*d), move(*d)) for d in everyone] for name, move in maps.items()}


def call(body, ins, outs, scratch=(), name=None):
    specs = [spec for spec, _ in ins]
    return pl.pallas_call(
        body,
        in_specs=specs,
        out_specs=[spec for spec, _ in outs],
        out_shape=[jax.ShapeDtypeStruct(shape, F32) for _, shape in outs],
        scratch_shapes=list(scratch),
        compiler_params=pltpu.CompilerParams(vmem_limit_bytes=8 << 20),
        name=name,
    )(*[value for _, value in ins])


def run_copies(copies, sems):
    started = [pltpu.make_async_copy(src, dst, sems.at[i]) for i, (src, dst) in enumerate(copies)]
    for copy in started:
        copy.start()
    for copy in started:
        copy.wait()


def pack_kernel(flags, field, *refs):
    coefs, (first, second, sems) = refs[:-3], refs[-3:]
    core, x = flags[0], flags[1]
    sections, rows = field.shape[1], first.shape[-2]
    step = field.shape[3] - rows
    copies = []
    for target, half in ((first, core), (second, 1 - core)):
        start = pl.multiple_of(half * step, SUB)
        for slot, plane in ((0, x), (1, 1 - x)):
            copies.append((field.at[0, :, plane, pl.ds(start, rows)], target.at[slot, pl.ds(0, sections)]))
    start = pl.multiple_of((1 - core) * step, SUB)
    for index, coef in enumerate(coefs):
        for slot, plane in ((0, x), (1, 1 - x)):
            copies.append((coef.at[plane, pl.ds(start, rows)], second.at[slot, sections + index]))
    run_copies(copies, sems)


def chunks(rows):
    return [(k, pl.ds(k * SUB, SUB)) for k in range(rows // SUB)]


def order_kernel(flags, weights, first, second, outer, inner, ends):
    x = flags[1]
    sections = outer.shape[1]
    for slot, target in ((0, outer), (1, inner)):
        for _, rows in chunks(outer.shape[2]):
            for s in range(sections):
                target[x, s, rows] = first[slot, s, rows]
                target[1 - x, s, rows] = second[slot, s, rows]
        for _, rows in chunks(outer.shape[2]):
            ends[slot, rows] = sum(weights[s] * target[1, s, rows] for s in range(sections))


def scale_kernel(flags, matrix, first, second, *outs):
    x = flags[1]
    sections = first.shape[1]
    for slot in range(2):
        source, coefs, fine, coarse = outs[4 * slot : 4 * slot + 4]
        for _, rows in chunks(first.shape[2]):
            for s in range(sections):
                source[x, s, rows] = first[slot, s, rows]
                source[1 - x, s, rows] = second[slot, s, rows]
            for index in range(3):
                coefs[index, rows] = second[slot, sections + index, rows]
            base = 6.0 * second[slot, sections, rows] + second[slot, sections + 1, rows]
            for s in range(sections):
                fine[s, rows] = 1.0 / (matrix[s, s] + base)
                coarse[s, rows] = 1.0 / (matrix[s, s] + 2.0 * base)


def edges():
    lane = lax.broadcasted_iota(jnp.int32, (SUB, 128), 1)
    row = lax.broadcasted_iota(jnp.int32, (SUB, 128), 0)
    return lane == 0, lane == 127, row == 0, row == SUB - 1


def around(read, total, k, center, masks):
    left, right, top, bottom = masks
    lanes = center.shape[1]
    near = jnp.where(left, 0.0, pltpu.roll(center, 1, 1)) + jnp.where(right, 0.0, pltpu.roll(center, lanes - 1, 1))
    if k == 0:
        above = jnp.where(top, 0.0, pltpu.roll(center, 1, 0))
    else:
        above = read(pl.ds(k * SUB - 1, SUB))
    if k == total - 1:
        below = jnp.where(bottom, 0.0, pltpu.roll(center, SUB - 1, 0))
    else:
        below = read(pl.ds(k * SUB + 1, SUB))
    return near + (above + below)


def off_mix(matrix, s, values):
    return sum(matrix[s, r] * values[r] for r in range(len(values)) if r != s)


def weighted(weights, values):
    return sum(weights[r] * value for r, value in enumerate(values))


def fine_kernel(flags, matrix, weights, field, other, halo, arrived, source, coefs, scale, *refs, slot, weight, last):
    total = field.shape[2] // SUB
    sections = field.shape[1]
    masks = edges()
    x, begins = flags[1], flags[2] == 1
    inside = flags[3].astype(F32)
    for k, rows in chunks(field.shape[2]):
        diffusion, reaction = coefs[0, rows], coefs[1, rows]
        values = [[field[n, s, rows] for s in range(sections)] for n in range(2)]
        befores = [jnp.where(begins, coefs[2, rows], arrived[slot, rows]), weighted(weights, values[0])]
        updated = []
        for n in range(2):
            for s in range(sections):
                value = values[n][s]
                beside = halo[n, s, rows]
                if slot == 0:
                    beside = beside * inside
                near = around(lambda at, n=n, s=s: field[n, s, at], total, k, value, masks)
                near = near + (other[n, s, rows] + beside)
                acc = (source[n, s, rows] + befores[n]) + diffusion * near
                acc = acc - off_mix(matrix, s, values[n]) - reaction * (jnp.tanh(value) - value)
                new = scale[s, rows] * acc
                if weight != 1.0:
                    new = (1.0 - weight) * value + weight * new
                updated.append(new)
        if not last:
            out = refs[-2]
            for n in range(2):
                for s in range(sections):
                    out[n, s, rows] = updated[n * sections + s]
            ends = weighted(weights, updated[sections:])
            if slot == 0:
                refs[-1][0, rows] = ends
                refs[-1][1, rows] = refs[0][rows]
            else:
                refs[-1][rows] = ends
        else:
            out = refs[-1]

            def put(rows=rows, k=k, updated=updated, out=out):
                place = pl.ds(pl.multiple_of((k - x) * SUB, SUB), SUB)
                for n in range(2):
                    for s in range(sections):
                        out[n, s, place] = updated[n * sections + s]

            if k == 0:
                pl.when(x == 0)(put)
            elif k == total - 1:
                pl.when(x == 1)(put)
            else:
                put()


def residual_kernel(flags, matrix, weights, field, other, halo, arrived, source, coefs, scale, *refs, slot):
    total = field.shape[2] // SUB
    sections = field.shape[1]
    masks = edges()
    begins = flags[2] == 1
    inside = flags[3].astype(F32)
    kept, out = refs[-3], refs[-2]
    for k, rows in chunks(field.shape[2]):
        diffusion, reaction = coefs[0, rows], coefs[1, rows]
        firsts = [field[0, s, rows] for s in range(sections)]
        seconds = [field[1, s, rows] for s in range(sections)]
        both = [a + b for a, b in zip(firsts, seconds)]
        before = jnp.where(begins, coefs[2, rows], arrived[slot, rows]) + weighted(weights, firsts)
        made = []
        for s in range(sections):
            beside = halo[0, s, rows] + halo[1, s, rows]
            if slot == 0:
                beside = beside * inside
            near = around(lambda at, s=s: field[0, s, at] + field[1, s, at], total, k, both[s], masks)
            near = near + (other[0, s, rows] + other[1, s, rows] + beside)
            acc = (source[0, s, rows] + source[1, s, rows]) + before + diffusion * (near - 6.0 * both[s])
            acc = acc - (off_mix(matrix, s, both) + matrix[s, s] * both[s])
            acc = acc - reaction * (jnp.tanh(firsts[s]) + jnp.tanh(seconds[s]))
            kept[s, rows] = acc
            new = 0.7 * (acc * scale[s, rows])
            out[s, rows] = new
            made.append(new)
        ends = weighted(weights, made)
        if slot == 0:
            refs[-1][0, rows] = ends
            refs[-1][1, rows] = refs[0][rows]
        else:
            refs[-1][rows] = ends


def coarse_kernel(flags, matrix, weights, field, other, halo, arrived, source, coefs, scale, *refs, slot, weight, last):
    total = field.shape[1] // SUB
    sections = field.shape[0]
    masks = edges()
    continues = flags[2] == 0
    inside = flags[3].astype(F32)
    for k, rows in chunks(field.shape[1]):
        double = 2.0 * coefs[0, rows]
        values = [field[s, rows] for s in range(sections)]
        before = jnp.where(continues, arrived[slot, rows], 0.0)
        made = []
        for s in range(sections):
            beside = halo[s, rows]
            if slot == 0:
                beside = beside * inside
            near = around(lambda at, s=s: field[s, at], total, k, values[s], masks)
            near = near + (other[s, rows] + beside)
            acc = (source[s, rows] + before) + double * near - off_mix(matrix, s, values)
            new = scale[s, rows] * acc
            if weight != 1.0:
                new = (1.0 - weight) * values[s] + weight * new
            made.append(new)
        out = refs[-2]
        if last:
            fine = refs[0]
            for n in range(2):
                for s in range(sections):
                    out[n, s, rows] = fine[n, s, rows] + made[s]
            made = [fine[1, s, rows] + made[s] for s in range(sections)]
        else:
            for s in range(sections):
                out[s, rows] = made[s]
        ends = weighted(weights, made)
        if slot == 0:
            refs[-1][0, rows] = ends
            refs[-1][1, rows] = refs[1 if last else 0][rows]
        else:
            refs[-1][rows] = ends


def split_kernel(flags, field, first, second):
    x = flags[1]
    for _, rows in chunks(field.shape[2]):
        for s in range(field.shape[1]):
            first[s, rows] = field[x, s, rows]
            second[s, rows] = field[1 - x, s, rows]


def place_kernel(flags, first_outer, second_outer, first_inner, second_inner, out, sems):
    core, x = flags[0], flags[1]
    half = first_outer.shape[1]
    copies = []
    for plane, parts in ((x, (first_outer, second_outer)), (1 - x, (first_inner, second_inner))):
        for part, which in zip(parts, (core, 1 - core)):
            start = pl.multiple_of(which * half, SUB)
            copies.append((part, out.at[0, :, plane, pl.ds(start, half)]))
    run_copies(copies, sems)


def local(state, source, start_field, diffusion, reaction, matrix, weights, moves):
    sections, ny, nz = state.shape[1], state.shape[3], state.shape[4]
    half = ny // 2
    rows = half + HALO
    tm, space = lax.axis_index("tm"), lax.axis_index("space")
    core, x = tm % 2, space % 2
    outermost = jnp.where(core == 0, space // 2 == 0, space // 2 == lax.axis_size("space") // 2 - 1)
    flags = jnp.stack([core, x, (tm // 2 == 0).astype(jnp.int32), 1 - outermost.astype(jnp.int32)]).astype(jnp.int32)

    def move(value, name):
        return lax.ppermute(value, ("tm", "space"), moves[name])

    small = [(SMEM, flags)]
    both = [(SMEM, flags), (SMEM, matrix), (SMEM, weights)]
    plane, pair = (sections, rows, nz), (2, sections, rows, nz)

    first, second = call(
        pack_kernel, small + [(ANY, state)], [(VMEM, (2, sections, rows, nz))] * 2, [pltpu.SemaphoreType.DMA((4,))], name="pack_state"
    )
    first, second = move(first, "first"), move(second, "second")
    more, rest = call(
        pack_kernel,
        small + [(ANY, source), (ANY, diffusion), (ANY, reaction), (ANY, start_field)],
        [(VMEM, (2, sections, rows, nz)), (VMEM, (2, sections + 3, rows, nz))],
        [pltpu.SemaphoreType.DMA((10,))],
        name="pack_source",
    )
    more, rest = move(more, "first"), move(rest, "second")
    outer, inner, ends = call(
        order_kernel,
        small + [(SMEM, weights), (VMEM, first), (VMEM, second)],
        [(VMEM, pair), (VMEM, pair), (VMEM, (2, rows, nz))],
        name="order",
    )
    source_o, coefs_o, fine_o, coarse_o, source_i, coefs_i, fine_i, coarse_i = call(
        scale_kernel,
        small + [(SMEM, matrix), (VMEM, more), (VMEM, rest)],
        [(VMEM, pair), (VMEM, (3, rows, nz)), (VMEM, plane), (VMEM, plane)] * 2,
        name="scale",
    )

    def step(body, outer, inner, ends, source_o, source_i, scale_o, scale_i, extra, outs, name):
        depth, beside, arrived = move(outer, "depth"), move(inner, "core"), move(ends, "time")
        made_i = call(
            functools.partial(body, slot=1),
            both + [(VMEM, v) for v in (inner, outer, beside, arrived, source_i, coefs_i, scale_i)] + [(VMEM, v) for v in extra[1]],
            [(VMEM, shape) for shape in outs] + [(VMEM, (rows, nz))],
            name=name + "_inner",
        )
        made_o = call(
            functools.partial(body, slot=0),
            both + [(VMEM, v) for v in (outer, inner, depth, arrived, source_o, coefs_o, scale_o)] + [(VMEM, v) for v in extra[0]] + [(VMEM, made_i[-1])],
            [(VMEM, shape) for shape in outs] + [(VMEM, (2, rows, nz))],
            name=name + "_outer",
        )
        return made_o, made_i

    none = ((), ())

    def fine(outer, inner, ends, weight):
        made_o, made_i = step(
            functools.partial(fine_kernel, weight=weight, last=False),
            outer, inner, ends, source_o, source_i, fine_o, fine_i, none, [pair], "fine",
        )
        return made_o[0], made_i[0], made_o[1]

    for weight in (0.6, 1.0):
        outer, inner, ends = fine(outer, inner, ends, weight)
    made_o, made_i = step(
        residual_kernel, outer, inner, ends, source_o, source_i, coarse_o, coarse_i, none, [plane, plane], "residual"
    )
    kept_o, kept_i = made_o[0], made_i[0]
    made_o, made_i = step(
        functools.partial(coarse_kernel, weight=1.0, last=False),
        made_o[1], made_i[1], made_o[2], kept_o, kept_i, coarse_o, coarse_i, none, [plane], "coarse",
    )
    made_o, made_i = step(
        functools.partial(coarse_kernel, weight=0.7, last=True),
        made_o[0], made_i[0], made_o[1], kept_o, kept_i, coarse_o, coarse_i, ((outer,), (inner,)), [pair], "coarse_last",
    )
    outer, inner, ends = fine(made_o[0], made_i[0], made_o[1], 1.0)

    depth, beside, arrived = move(outer, "depth"), move(inner, "core"), move(ends, "time")
    body = functools.partial(fine_kernel, weight=0.6, last=True)
    parts = []
    for slot, args in ((1, (inner, outer, beside, arrived, source_i, coefs_i, fine_i)), (0, (outer, inner, depth, arrived, source_o, coefs_o, fine_o))):
        (made,) = call(
            functools.partial(body, slot=slot), both + [(VMEM, v) for v in args], [(VMEM, (2, sections, half, nz))], name=f"last_{slot}"
        )
        first, second = call(split_kernel, small + [(VMEM, made)], [(VMEM, (sections, half, nz))] * 2, name=f"split_{slot}")
        parts.append((move(first, "first"), move(second, "back")))
    (out,) = call(
        place_kernel, small + [(VMEM, v) for v in parts[1] + parts[0]], [(ANY, state.shape)], [pltpu.SemaphoreType.DMA((4,))], name="place"
    )
    return out


def solution(mesh):
    moves = permutations(mesh.shape["tm"], mesh.shape["space"])
    in_specs = (
        P("tm", None, "space", None, None),
        P("tm", None, "space", None, None),
        P("space", None, None),
        P("space", None, None),
        P("space", None, None),
        P(),
        P(),
    )
    out_specs = P("tm", None, "space", None, None)
    body = functools.partial(local, moves=moves)
    return jax.shard_map(body, mesh=mesh, in_specs=in_specs, out_specs=out_specs, check_vma=False)
```

```python
import functools

import jax
import jax.numpy as jnp
from jax import lax
from jax.experimental import pallas as pl
from jax.experimental.pallas import tpu as pltpu
from jax.sharding import PartitionSpec as P


HALO = 8
SUB = 8

VMEM = pl.BlockSpec(memory_space=pltpu.VMEM)
HBM = pl.BlockSpec(memory_space=pltpu.HBM)
F32 = jnp.float32


def permutations(slabs, blocks):
    ys, zs = slabs // 2, blocks // 2

    def at(y, c, z, x):
        return (2 * y + c) * blocks + 2 * z + x

    everyone = [(y, c, z, x) for y in range(ys) for c in range(2) for z in range(zs) for x in range(2)]

    def depth(y, c, z, x, edge):
        if c == 1:
            return at(y, 0, z + 1, x) if z + 1 < zs else edge
        return at(y, 1, z - 1, x) if z > 0 else edge

    maps = {
        "first": lambda y, c, z, x: at(y, x, z, c),
        "second": lambda y, c, z, x: at(y, x, z, 1 - c),
        "back": lambda y, c, z, x: at(y, 1 - x, z, c),
        "depth": lambda y, c, z, x: depth(y, c, z, x, at(y, c, z, 1 - x)),
        "depth_early": lambda y, c, z, x: depth(y, c, z, x, at(y ^ 1 if y ^ 1 < ys else y, c, z, x)),
        "core": lambda y, c, z, x: at(y, 1 - c, z, x),
        "time": lambda y, c, z, x: at((y + 1) % ys, c, z, x),
    }
    return {name: [(at(*d), move(*d)) for d in everyone] for name, move in maps.items()}


def call(body, ins, outs, scratch=()):
    specs = [spec for spec, _ in ins]
    return pl.pallas_call(
        body,
        in_specs=specs,
        out_specs=[spec for spec, _ in outs],
        out_shape=[jax.ShapeDtypeStruct(shape, F32) for _, shape in outs],
        scratch_shapes=list(scratch),
        compiler_params=pltpu.CompilerParams(vmem_limit_bytes=8 << 20),
    )(*[value for _, value in ins])


def run_copies(copies, sems):
    started = [pltpu.make_async_copy(src, dst, sems.at[i]) for i, (src, dst) in enumerate(copies)]
    for copy in started:
        copy.start()
    for copy in started:
        copy.wait()


def place_of():
    return lax.axis_index("tm") % 2, lax.axis_index("space") % 2


def pack_kernel(*refs):
    fields, (first, second, sems) = refs[:-3], refs[-3:]
    core, x = place_of()
    field = fields[0]
    sections, rows = field.shape[1], first.shape[-2]
    step = field.shape[3] - rows
    near = pl.ds(pl.multiple_of(core * step, SUB), rows)
    far = pl.ds(pl.multiple_of((1 - core) * step, SUB), rows)
    copies = []
    for slot, plane in enumerate((x, 1 - x)):
        copies.append((field.at[0, :, plane, near], first.at[slot]))
        copies.append((field.at[0, :, plane, far], second.at[slot, pl.ds(0, sections)]))
        for index, coef in enumerate(fields[1:]):
            copies.append((coef.at[plane, far], second.at[slot, sections + index]))
    run_copies(copies, sems)


def chunks(rows):
    return [(k, pl.ds(k * SUB, SUB)) for k in range(rows // SUB)]


class Table:
    def __init__(self, ref, sections):
        self.ref, self.sections = ref, sections

    def matrix(self, s, r):
        return self.ref[s * self.sections + r]

    def weight(self, r):
        return self.ref[self.sections * self.sections + r]

    def mask(self, index):
        return self.ref[self.sections * (self.sections + 1) + index]

    def off_mix(self, s, values):
        return sum(self.matrix(s, r) * values[r] for r in range(self.sections) if r != s)

    def weighted(self, values):
        return sum(self.weight(r) * value for r, value in enumerate(values))


CONTINUES, INSIDE, LEFT = range(3)


def table_of(matrix, weights):
    tm, space = lax.axis_index("tm"), lax.axis_index("space")
    depth, x = space // 2, space % 2
    edge = jnp.where(tm % 2 == 0, 0, lax.axis_size("space") // 2 - 1)
    masks = jnp.stack([tm // 2 != 0, depth != edge, x == 0]).astype(F32)
    flat = jnp.concatenate([matrix.reshape(-1), weights, masks])
    return jnp.broadcast_to(flat[:, None, None], (flat.shape[0], SUB, 128))


def order_kernel(table, first, second, outer, inner, ends):
    sections = outer.shape[1]
    params = Table(table, sections)
    left = params.mask(LEFT) > 0.5
    for slot, field in enumerate((outer, inner)):
        for _, rows in chunks(field.shape[2]):
            later = []
            for s in range(sections):
                a, b = first[slot, s, rows], second[slot, s, rows]
                field[0, s, rows] = jnp.where(left, a, b)
                later.append(jnp.where(left, b, a))
                field[1, s, rows] = later[-1]
            ends[slot, rows] = params.weighted(later)


def put_ends(refs, rows, ends, slot):
    if slot == 0:
        refs[-1][0, rows] = ends
        refs[-1][1, rows] = refs[0][rows]
    else:
        refs[-1][rows] = ends


def scale_kernel(table, first, second, *outs):
    sections = first.shape[1]
    params = Table(table, sections)
    left = params.mask(LEFT) > 0.5
    begins = 1.0 - params.mask(CONTINUES)
    for slot in range(2):
        source, coefs, fine, coarse = outs[4 * slot : 4 * slot + 4]
        for _, rows in chunks(first.shape[2]):
            for s in range(sections):
                a, b = first[slot, s, rows], second[slot, s, rows]
                source[0, s, rows] = jnp.where(left, a, b)
                source[1, s, rows] = jnp.where(left, b, a)
            diffusion, reaction = second[slot, sections, rows], second[slot, sections + 1, rows]
            coefs[0, rows] = diffusion
            coefs[1, rows] = reaction
            coefs[2, rows] = begins * second[slot, sections + 2, rows]
            base = 6.0 * diffusion + reaction
            for s in range(sections):
                fine[s, rows] = 1.0 / (params.matrix(s, s) + base)
                coarse[s, rows] = 1.0 / (params.matrix(s, s) + 2.0 * base)


def edges():
    lane = lax.broadcasted_iota(jnp.int32, (SUB, 128), 1)
    row = lax.broadcasted_iota(jnp.int32, (SUB, 128), 0)
    return lane == 0, lane == 127, row == 0, row == SUB - 1


def around(read, total, k, center, masks):
    left, right, top, bottom = masks
    lanes = center.shape[1]
    near = jnp.where(left, 0.0, pltpu.roll(center, 1, 1)) + jnp.where(right, 0.0, pltpu.roll(center, lanes - 1, 1))
    if k == 0:
        above = jnp.where(top, 0.0, pltpu.roll(center, 1, 0))
    else:
        above = read(pl.ds(k * SUB - 1, SUB))
    if k == total - 1:
        below = jnp.where(bottom, 0.0, pltpu.roll(center, SUB - 1, 0))
    else:
        below = read(pl.ds(k * SUB + 1, SUB))
    return near + (above + below)


def fine_kernel(table, field, other, halo, arrived, source, coefs, scale, *refs, slot, weight, last, sums=False, parts=False):
    total = field.shape[2] // SUB
    sections = field.shape[1]
    params = Table(table, sections)
    masks = edges()
    left = params.mask(LEFT) > 0.5
    x = place_of()[1] if last else None
    for k, rows in chunks(field.shape[2]):
        diffusion, reaction = coefs[0, rows], coefs[1, rows]
        values = [[field[n, s, rows] for s in range(sections)] for n in range(2)]
        befores = [coefs[2, rows] + params.mask(CONTINUES) * arrived[slot, rows], params.weighted(values[0])]
        updated = []
        for n in range(2):
            for s in range(sections):
                value = values[n][s]
                if slot == 1 or not parts:
                    beside = halo[n, s, rows]
                elif n == 0:
                    beside = refs[1][s, rows] + halo[s, rows]
                else:
                    beside = refs[2][s, rows] - refs[1][s, rows] + halo[s, rows]
                if slot == 0:
                    beside = beside * params.mask(INSIDE)
                near = around(lambda at, n=n, s=s: field[n, s, at], total, k, value, masks)
                near = near + (other[n, s, rows] + beside)
                acc = (source[n, s, rows] + befores[n]) + diffusion * near
                acc = acc - params.off_mix(s, values[n]) - reaction * (jnp.tanh(value) - value)
                new = scale[s, rows] * acc
                if weight != 1.0:
                    new = (1.0 - weight) * value + weight * new
                updated.append(new)
        if not last:
            out = refs[-4 if sums and slot == 0 else -2]
            for n in range(2):
                for s in range(sections):
                    out[n, s, rows] = updated[n * sections + s]
            if sums and slot == 0:
                for s in range(sections):
                    refs[-3][s, rows] = updated[s] + updated[sections + s]
                    refs[-2][s, rows] = updated[s]
            put_ends(refs, rows, params.weighted(updated[sections:]), slot)
        else:

            def put(k=k, updated=updated):
                place = pl.ds(pl.multiple_of((k - x) * SUB, SUB), SUB)
                for s in range(sections):
                    a, b = updated[s], updated[sections + s]
                    refs[0][s, place] = jnp.where(left, a, b)
                    refs[1][s, place] = jnp.where(left, b, a)

            if k == 0:
                pl.when(x == 0)(put)
            elif k == total - 1:
                pl.when(x == 1)(put)
            else:
                put()


def residual_kernel(table, field, other, halo, arrived, source, coefs, scale, *refs, slot):
    total = field.shape[2] // SUB
    sections = field.shape[1]
    params = Table(table, sections)
    masks = edges()
    kept, out = refs[-3], refs[-2]
    for k, rows in chunks(field.shape[2]):
        diffusion, reaction = coefs[0, rows], coefs[1, rows]
        firsts = [field[0, s, rows] for s in range(sections)]
        seconds = [field[1, s, rows] for s in range(sections)]
        both = [a + b for a, b in zip(firsts, seconds)]
        before = coefs[2, rows] + params.mask(CONTINUES) * arrived[slot, rows] + params.weighted(firsts)
        made = []
        for s in range(sections):
            if slot == 0:
                beside = halo[s, rows] * params.mask(INSIDE)
            else:
                beside = halo[0, s, rows] + halo[1, s, rows]
            near = around(lambda at, s=s: field[0, s, at] + field[1, s, at], total, k, both[s], masks)
            near = near + (other[0, s, rows] + other[1, s, rows] + beside)
            acc = (source[0, s, rows] + source[1, s, rows]) + before + diffusion * (near - 6.0 * both[s])
            acc = acc - (params.off_mix(s, both) + params.matrix(s, s) * both[s])
            acc = acc - reaction * (jnp.tanh(firsts[s]) + jnp.tanh(seconds[s]))
            kept[s, rows] = acc
            new = 0.7 * (acc * scale[s, rows])
            out[s, rows] = new
            made.append(new)
        put_ends(refs, rows, params.weighted(made), slot)


def coarse_kernel(table, field, other, halo, arrived, source, coefs, scale, *refs, slot, weight, last):
    total = field.shape[1] // SUB
    sections = field.shape[0]
    params = Table(table, sections)
    masks = edges()
    out = refs[-2]
    for k, rows in chunks(field.shape[1]):
        double = 2.0 * coefs[0, rows]
        values = [field[s, rows] for s in range(sections)]
        before = params.mask(CONTINUES) * arrived[slot, rows]
        made = []
        for s in range(sections):
            beside = halo[s, rows]
            if slot == 0:
                beside = beside * params.mask(INSIDE)
            near = around(lambda at, s=s: field[s, at], total, k, values[s], masks)
            near = near + (other[s, rows] + beside)
            acc = (source[s, rows] + before) + double * near - params.off_mix(s, values)
            new = scale[s, rows] * acc
            if weight != 1.0:
                new = (1.0 - weight) * values[s] + weight * new
            made.append(new)
        if last:
            fine = refs[-4 if slot == 0 else -3]
            if slot == 0:
                out = refs[-3]
                for s in range(sections):
                    refs[-2][s, rows] = made[s]
            for n in range(2):
                for s in range(sections):
                    out[n, s, rows] = fine[n, s, rows] + made[s]
            made = [fine[1, s, rows] + made[s] for s in range(sections)]
        else:
            for s in range(sections):
                out[s, rows] = made[s]
        put_ends(refs, rows, params.weighted(made), slot)


def place_kernel(first_outer, second_outer, first_inner, second_inner, out, sems):
    core, x = place_of()
    half = first_outer.shape[1]
    copies = []
    for plane, parts in ((x, (first_outer, second_outer)), (1 - x, (first_inner, second_inner))):
        for part, which in zip(parts, (core, 1 - core)):
            start = pl.multiple_of(which * half, SUB)
            copies.append((part, out.at[0, :, plane, pl.ds(start, half)]))
    run_copies(copies, sems)


def local(state, source, start_field, diffusion, reaction, matrix, weights, moves):
    sections, ny, nz = state.shape[1], state.shape[3], state.shape[4]
    half = ny // 2
    rows = half + HALO
    plane, pair = (sections, rows, nz), (2, sections, rows, nz)
    single, double = (rows, nz), (2, rows, nz)

    def move(value, name):
        return lax.ppermute(value, ("tm", "space"), moves[name])

    def within(*values):
        return [(VMEM, v) for v in values]

    def pack(fields):
        first, second = call(
            pack_kernel,
            [(HBM, pltpu.with_memory_space_constraint(v, pltpu.HBM)) for v in fields],
            within(pair, (2, sections + len(fields) - 1, rows, nz)),
            [pltpu.SemaphoreType.DMA((2 * len(fields) + 2,))],
        )
        return move(first, "first"), move(second, "second")

    states = pack((state,))
    given = pack((source, diffusion, reaction, start_field))
    table = table_of(matrix, weights)
    outer, inner, ends = call(order_kernel, within(table, *states), within(pair, pair, double))
    kept = call(scale_kernel, within(table, *given), within(pair, (3, rows, nz), plane, plane) * 2)
    sources, coefs, fines, coarses = zip(kept[:4], kept[4:])

    def exchange(sent, inner, ends, name):
        depth = move(sent, "depth_early" if name == "fine_0" else "depth")
        arrived = move(ends, "time")
        return depth, move(inner, "core"), arrived

    def step(body, fields, sent, ends, source, scale, outs, name, extra=((), ()), more_outs=()):
        outer, inner = fields
        depth, beside, arrived = exchange(sent, inner, ends, name)
        halos[name] = depth

        def half_step(slot, own, other, halo, *more):
            return call(
                functools.partial(body, slot=slot),
                within(table, own, other, halo, arrived, source[slot], coefs[slot], scale[slot], *more, *extra[slot]),
                within(*outs, *(more_outs if slot == 0 else ()), single if slot else double),
            )

        made = half_step(1, inner, outer, beside)
        made_o = half_step(0, outer, inner, depth, made[-1])
        return list(zip(made_o, made[:-1])), made_o[len(outs) : -1], made_o[-1]

    def fine(weight, **options):
        return functools.partial(fine_kernel, weight=weight, last=False, **options)

    halos = {}
    fields = (outer, inner)
    (fields,), _, ends = step(fine(0.6), fields, outer, ends, sources, fines, [pair], "fine_0")
    (fields,), (both, first), ends = step(
        fine(1.0, sums=True), fields, fields[0], ends, sources, fines, [pair], "fine_1", more_outs=(plane, plane)
    )
    (kept, coarse), _, ends = step(residual_kernel, fields, both, ends, sources, coarses, [plane, plane], "residual")
    first, both = move(first, "depth"), halos["residual"]
    body = functools.partial(coarse_kernel, weight=1.0, last=False)
    (coarse,), _, ends = step(body, coarse, coarse[0], ends, kept, coarses, [plane], "coarse")
    body = functools.partial(coarse_kernel, weight=0.7, last=True)
    (fields,), (change,), ends = step(
        body, coarse, coarse[0], ends, kept, coarses, [pair], "correct", extra=[(f,) for f in fields], more_outs=(plane,)
    )
    (fields,), _, ends = step(
        fine(1.0, parts=True), fields, change, ends, sources, fines, [pair], "fine_2", extra=((first, both), ())
    )
    outer, inner = fields

    depth, beside, arrived = exchange(outer, inner, ends, "last")
    body = functools.partial(fine_kernel, weight=0.6, last=True)
    parts = []
    for slot, own, other, halo in ((1, inner, outer, beside), (0, outer, inner, depth)):
        first, second = call(
            functools.partial(body, slot=slot),
            within(table, own, other, halo, arrived, sources[slot], coefs[slot], fines[slot]),
            within(*[(sections, half, nz)] * 2),
        )
        parts.append((move(first, "first"), move(second, "back")))
    (out,) = call(place_kernel, within(*parts[1], *parts[0]), [(HBM, state.shape)], [pltpu.SemaphoreType.DMA((4,))])
    return out


def solution(mesh):
    moves = permutations(mesh.shape["tm"], mesh.shape["space"])
    in_specs = (
        P("tm", None, "space", None, None),
        P("tm", None, "space", None, None),
        P("space", None, None),
        P("space", None, None),
        P("space", None, None),
        P(),
        P(),
    )
    out_specs = P("tm", None, "space", None, None)

    def body(*args):
        return local(*args, moves=moves)

    return jax.shard_map(body, mesh=mesh, in_specs=in_specs, out_specs=out_specs, check_vma=False)
```

```python
import functools

import jax
import jax.numpy as jnp
from jax import lax
from jax.experimental import pallas as pl
from jax.experimental.pallas import tpu as pltpu
from jax.sharding import PartitionSpec as P


HALO = 8
SUB = 8

VMEM = pl.BlockSpec(memory_space=pltpu.VMEM)
SMEM = pl.BlockSpec(memory_space=pltpu.SMEM)
HBM = pl.BlockSpec(memory_space=pltpu.HBM)
F32 = jnp.float32


def permutations(slabs, blocks):
    ys, zs = slabs // 2, blocks // 2

    def at(y, c, z, x):
        return (2 * y + c) * blocks + 2 * z + x

    everyone = [(y, c, z, x) for y in range(ys) for c in range(2) for z in range(zs) for x in range(2)]

    def depth(y, c, z, x, edge):
        if c == 1:
            return at(y, 0, z + 1, x) if z + 1 < zs else edge
        return at(y, 1, z - 1, x) if z > 0 else edge

    maps = {
        "first": lambda y, c, z, x: at(y, x, z, c),
        "second": lambda y, c, z, x: at(y, x, z, 1 - c),
        "back": lambda y, c, z, x: at(y, 1 - x, z, c),
        "depth": lambda y, c, z, x: depth(y, c, z, x, at(y, c, z, 1 - x)),
        "depth_early": lambda y, c, z, x: depth(y, c, z, x, at(y ^ 1 if y ^ 1 < ys else y, c, z, x)),
        "core": lambda y, c, z, x: at(y, 1 - c, z, x),
        "time": lambda y, c, z, x: at((y + 1) % ys, c, z, x),
    }
    return {name: [(at(*d), move(*d)) for d in everyone] for name, move in maps.items()}


def call(body, ins, outs, scratch=()):
    specs = [spec for spec, _ in ins]
    return pl.pallas_call(
        body,
        in_specs=specs,
        out_specs=[spec for spec, _ in outs],
        out_shape=[jax.ShapeDtypeStruct(shape, F32) for _, shape in outs],
        scratch_shapes=list(scratch),
        compiler_params=pltpu.CompilerParams(vmem_limit_bytes=8 << 20),
    )(*[value for _, value in ins])


def run_copies(copies, sems):
    started = [pltpu.make_async_copy(src, dst, sems.at[i]) for i, (src, dst) in enumerate(copies)]
    for copy in started:
        copy.start()
    for copy in started:
        copy.wait()


def place_of():
    return lax.axis_index("tm") % 2, lax.axis_index("space") % 2


def pack_kernel(*refs):
    fields, (first, second, sems) = refs[:-3], refs[-3:]
    core, x = place_of()
    field = fields[0]
    sections, rows = field.shape[1], first.shape[-2]
    step = field.shape[3] - rows
    near = pl.ds(pl.multiple_of(core * step, SUB), rows)
    far = pl.ds(pl.multiple_of((1 - core) * step, SUB), rows)
    copies = []
    for slot, plane in enumerate((x, 1 - x)):
        copies.append((field.at[0, :, plane, near], first.at[slot]))
        copies.append((field.at[0, :, plane, far], second.at[slot, pl.ds(0, sections)]))
        for index, coef in enumerate(fields[1:]):
            copies.append((coef.at[plane, far], second.at[slot, sections + index]))
    run_copies(copies, sems)


def chunks(rows):
    return [(k, pl.ds(k * SUB, SUB)) for k in range(rows // SUB)]


class Table:
    def __init__(self, ref, sections):
        self.ref, self.sections = ref, sections

    def matrix(self, s, r):
        return self.ref[s * self.sections + r]

    def weight(self, r):
        return self.ref[self.sections * self.sections + r]

    def mask(self, index):
        return self.ref[self.sections * (self.sections + 1) + index]

    def off_mix(self, s, values):
        return sum(self.matrix(s, r) * values[r] for r in range(self.sections) if r != s)

    def weighted(self, values):
        return sum(self.weight(r) * value for r, value in enumerate(values))


CONTINUES, INSIDE, LEFT = range(3)


def table_kernel(matrix, weights, table):
    tm, space = lax.axis_index("tm"), lax.axis_index("space")
    edge = jnp.where(tm % 2 == 0, 0, lax.axis_size("space") // 2 - 1)
    sections = weights.shape[0]
    flat = [matrix[s, r] for s in range(sections) for r in range(sections)]
    flat += [weights[r] for r in range(sections)]
    flat += [jnp.where(mask, 1.0, 0.0) for mask in (tm // 2 != 0, space // 2 != edge, space % 2 == 0)]
    for index, value in enumerate(flat):
        table[index] = jnp.full(table.shape[1:], value, F32)


def order_kernel(table, first, second, outer, inner, ends):
    sections = outer.shape[1]
    params = Table(table, sections)
    left = params.mask(LEFT) > 0.5
    for slot, field in enumerate((outer, inner)):
        for _, rows in chunks(field.shape[2]):
            later = []
            for s in range(sections):
                a, b = first[slot, s, rows], second[slot, s, rows]
                field[0, s, rows] = jnp.where(left, a, b)
                later.append(jnp.where(left, b, a))
                field[1, s, rows] = later[-1]
            ends[slot, rows] = params.weighted(later)


def put_ends(refs, rows, ends, slot):
    if slot == 0:
        refs[-1][0, rows] = ends
        refs[-1][1, rows] = refs[0][rows]
    else:
        refs[-1][rows] = ends


def scale_kernel(table, first, second, *outs):
    sections = first.shape[1]
    params = Table(table, sections)
    left = params.mask(LEFT) > 0.5
    begins = 1.0 - params.mask(CONTINUES)
    for slot in range(2):
        source, coefs, fine, coarse = outs[4 * slot : 4 * slot + 4]
        for _, rows in chunks(first.shape[2]):
            for s in range(sections):
                a, b = first[slot, s, rows], second[slot, s, rows]
                source[0, s, rows] = jnp.where(left, a, b)
                source[1, s, rows] = jnp.where(left, b, a)
            diffusion, reaction = second[slot, sections, rows], second[slot, sections + 1, rows]
            coefs[0, rows] = diffusion
            coefs[1, rows] = reaction
            coefs[2, rows] = begins * second[slot, sections + 2, rows]
            base = 6.0 * diffusion + reaction
            for s in range(sections):
                fine[s, rows] = 1.0 / (params.matrix(s, s) + base)
                coarse[s, rows] = 1.0 / (params.matrix(s, s) + 2.0 * base)


def edges():
    lane = lax.broadcasted_iota(jnp.int32, (SUB, 128), 1)
    row = lax.broadcasted_iota(jnp.int32, (SUB, 128), 0)
    return lane == 0, lane == 127, row == 0, row == SUB - 1


def around(read, total, k, center, masks):
    left, right, top, bottom = masks
    lanes = center.shape[1]
    near = jnp.where(left, 0.0, pltpu.roll(center, 1, 1)) + jnp.where(right, 0.0, pltpu.roll(center, lanes - 1, 1))
    if k == 0:
        above = jnp.where(top, 0.0, pltpu.roll(center, 1, 0))
    else:
        above = read(pl.ds(k * SUB - 1, SUB))
    if k == total - 1:
        below = jnp.where(bottom, 0.0, pltpu.roll(center, SUB - 1, 0))
    else:
        below = read(pl.ds(k * SUB + 1, SUB))
    return near + (above + below)


def fine_kernel(table, field, other, halo, arrived, source, coefs, scale, *refs, slot, weight, last, sums=False, parts=False):
    total = field.shape[2] // SUB
    sections = field.shape[1]
    params = Table(table, sections)
    masks = edges()
    left = params.mask(LEFT) > 0.5
    x = place_of()[1] if last else None
    for k, rows in chunks(field.shape[2]):
        diffusion, reaction = coefs[0, rows], coefs[1, rows]
        values = [[field[n, s, rows] for s in range(sections)] for n in range(2)]
        befores = [coefs[2, rows] + params.mask(CONTINUES) * arrived[slot, rows], params.weighted(values[0])]
        updated = []
        for n in range(2):
            for s in range(sections):
                value = values[n][s]
                if slot == 1 or not parts:
                    beside = halo[n, s, rows]
                elif n == 0:
                    beside = refs[1][s, rows] + halo[s, rows]
                else:
                    beside = refs[2][s, rows] - refs[1][s, rows] + halo[s, rows]
                if slot == 0:
                    beside = beside * params.mask(INSIDE)
                near = around(lambda at, n=n, s=s: field[n, s, at], total, k, value, masks)
                near = near + (other[n, s, rows] + beside)
                acc = (source[n, s, rows] + befores[n]) + diffusion * near
                acc = acc - params.off_mix(s, values[n]) - reaction * (jnp.tanh(value) - value)
                new = scale[s, rows] * acc
                if weight != 1.0:
                    new = (1.0 - weight) * value + weight * new
                updated.append(new)
        if not last:
            out = refs[-4 if sums and slot == 0 else -2]
            for n in range(2):
                for s in range(sections):
                    out[n, s, rows] = updated[n * sections + s]
            if sums and slot == 0:
                for s in range(sections):
                    refs[-3][s, rows] = updated[s] + updated[sections + s]
                    refs[-2][s, rows] = updated[s]
            put_ends(refs, rows, params.weighted(updated[sections:]), slot)
        else:

            def put(k=k, updated=updated):
                place = pl.ds(pl.multiple_of((k - x) * SUB, SUB), SUB)
                for s in range(sections):
                    a, b = updated[s], updated[sections + s]
                    refs[0][s, place] = jnp.where(left, a, b)
                    refs[1][s, place] = jnp.where(left, b, a)

            if k == 0:
                pl.when(x == 0)(put)
            elif k == total - 1:
                pl.when(x == 1)(put)
            else:
                put()


def residual_kernel(table, field, other, halo, arrived, source, coefs, scale, *refs, slot):
    total = field.shape[2] // SUB
    sections = field.shape[1]
    params = Table(table, sections)
    masks = edges()
    kept, out = refs[-3], refs[-2]
    for k, rows in chunks(field.shape[2]):
        diffusion, reaction = coefs[0, rows], coefs[1, rows]
        firsts = [field[0, s, rows] for s in range(sections)]
        seconds = [field[1, s, rows] for s in range(sections)]
        both = [a + b for a, b in zip(firsts, seconds)]
        before = coefs[2, rows] + params.mask(CONTINUES) * arrived[slot, rows] + params.weighted(firsts)
        made = []
        for s in range(sections):
            if slot == 0:
                beside = halo[s, rows] * params.mask(INSIDE)
            else:
                beside = halo[0, s, rows] + halo[1, s, rows]
            near = around(lambda at, s=s: field[0, s, at] + field[1, s, at], total, k, both[s], masks)
            near = near + (other[0, s, rows] + other[1, s, rows] + beside)
            acc = (source[0, s, rows] + source[1, s, rows]) + before + diffusion * (near - 6.0 * both[s])
            acc = acc - (params.off_mix(s, both) + params.matrix(s, s) * both[s])
            acc = acc - reaction * (jnp.tanh(firsts[s]) + jnp.tanh(seconds[s]))
            kept[s, rows] = acc
            new = 0.7 * (acc * scale[s, rows])
            out[s, rows] = new
            made.append(new)
        put_ends(refs, rows, params.weighted(made), slot)


def coarse_kernel(table, field, other, halo, arrived, source, coefs, scale, *refs, slot, weight, last):
    total = field.shape[1] // SUB
    sections = field.shape[0]
    params = Table(table, sections)
    masks = edges()
    out = refs[-2]
    for k, rows in chunks(field.shape[1]):
        double = 2.0 * coefs[0, rows]
        values = [field[s, rows] for s in range(sections)]
        before = params.mask(CONTINUES) * arrived[slot, rows]
        made = []
        for s in range(sections):
            beside = halo[s, rows]
            if slot == 0:
                beside = beside * params.mask(INSIDE)
            near = around(lambda at, s=s: field[s, at], total, k, values[s], masks)
            near = near + (other[s, rows] + beside)
            acc = (source[s, rows] + before) + double * near - params.off_mix(s, values)
            new = scale[s, rows] * acc
            if weight != 1.0:
                new = (1.0 - weight) * values[s] + weight * new
            made.append(new)
        if last:
            fine = refs[-4 if slot == 0 else -3]
            if slot == 0:
                out = refs[-3]
                for s in range(sections):
                    refs[-2][s, rows] = made[s]
            for n in range(2):
                for s in range(sections):
                    out[n, s, rows] = fine[n, s, rows] + made[s]
            made = [fine[1, s, rows] + made[s] for s in range(sections)]
        else:
            for s in range(sections):
                out[s, rows] = made[s]
        put_ends(refs, rows, params.weighted(made), slot)


def place_kernel(first_outer, second_outer, first_inner, second_inner, out, sems):
    core, x = place_of()
    half = first_outer.shape[1]
    copies = []
    for plane, parts in ((x, (first_outer, second_outer)), (1 - x, (first_inner, second_inner))):
        for part, which in zip(parts, (core, 1 - core)):
            start = pl.multiple_of(which * half, SUB)
            copies.append((part, out.at[0, :, plane, pl.ds(start, half)]))
    run_copies(copies, sems)


def local(state, source, start_field, diffusion, reaction, matrix, weights, moves):
    sections, ny, nz = state.shape[1], state.shape[3], state.shape[4]
    half = ny // 2
    rows = half + HALO
    plane, pair = (sections, rows, nz), (2, sections, rows, nz)
    single, double = (rows, nz), (2, rows, nz)

    def move(value, name):
        return lax.ppermute(value, ("tm", "space"), moves[name])

    def within(*values):
        return [(VMEM, v) for v in values]

    def pack(fields):
        first, second = call(
            pack_kernel,
            [(HBM, pltpu.with_memory_space_constraint(v, pltpu.HBM)) for v in fields],
            within(pair, (2, sections + len(fields) - 1, rows, nz)),
            [pltpu.SemaphoreType.DMA((2 * len(fields) + 2,))],
        )
        return move(first, "first"), move(second, "second")

    states = pack((state,))
    given = pack((source, diffusion, reaction, start_field))
    given_parameters = [(SMEM, matrix), (SMEM, weights)]
    (table,) = call(table_kernel, given_parameters, within((sections * (sections + 1) + 3, SUB, 128)))
    outer, inner, ends = call(order_kernel, within(table, *states), within(pair, pair, double))
    kept = call(scale_kernel, within(table, *given), within(pair, (3, rows, nz), plane, plane) * 2)
    sources, coefs, fines, coarses = zip(kept[:4], kept[4:])

    def exchange(sent, inner, ends, name):
        depth = move(sent, "depth_early" if name == "fine_0" else "depth")
        arrived = move(ends, "time")
        return depth, move(inner, "core"), arrived

    def step(body, fields, sent, ends, source, scale, outs, name, extra=((), ()), more_outs=()):
        outer, inner = fields
        depth, beside, arrived = exchange(sent, inner, ends, name)
        halos[name] = depth

        def half_step(slot, own, other, halo, *more):
            return call(
                functools.partial(body, slot=slot),
                within(table, own, other, halo, arrived, source[slot], coefs[slot], scale[slot], *more, *extra[slot]),
                within(*outs, *(more_outs if slot == 0 else ()), single if slot else double),
            )

        made = half_step(1, inner, outer, beside)
        made_o = half_step(0, outer, inner, depth, made[-1])
        return list(zip(made_o, made[:-1])), made_o[len(outs) : -1], made_o[-1]

    def fine(weight, **options):
        return functools.partial(fine_kernel, weight=weight, last=False, **options)

    halos = {}
    fields = (outer, inner)
    (fields,), _, ends = step(fine(0.6), fields, outer, ends, sources, fines, [pair], "fine_0")
    (fields,), (both, first), ends = step(
        fine(1.0, sums=True), fields, fields[0], ends, sources, fines, [pair], "fine_1", more_outs=(plane, plane)
    )
    (kept, coarse), _, ends = step(residual_kernel, fields, both, ends, sources, coarses, [plane, plane], "residual")
    first, both = move(first, "depth"), halos["residual"]
    body = functools.partial(coarse_kernel, weight=1.0, last=False)
    (coarse,), _, ends = step(body, coarse, coarse[0], ends, kept, coarses, [plane], "coarse")
    body = functools.partial(coarse_kernel, weight=0.7, last=True)
    (fields,), (change,), ends = step(
        body, coarse, coarse[0], ends, kept, coarses, [pair], "correct", extra=[(f,) for f in fields], more_outs=(plane,)
    )
    (fields,), _, ends = step(
        fine(1.0, parts=True), fields, change, ends, sources, fines, [pair], "fine_2", extra=((first, both), ())
    )
    outer, inner = fields

    depth, beside, arrived = exchange(outer, inner, ends, "last")
    body = functools.partial(fine_kernel, weight=0.6, last=True)
    parts = []
    for slot, own, other, halo in ((1, inner, outer, beside), (0, outer, inner, depth)):
        first, second = call(
            functools.partial(body, slot=slot),
            within(table, own, other, halo, arrived, sources[slot], coefs[slot], fines[slot]),
            within(*[(sections, half, nz)] * 2),
        )
        parts.append((move(first, "first"), move(second, "back")))
    (out,) = call(place_kernel, within(*parts[1], *parts[0]), [(HBM, state.shape)], [pltpu.SemaphoreType.DMA((4,))])
    return out


def solution(mesh):
    moves = permutations(mesh.shape["tm"], mesh.shape["space"])
    in_specs = (
        P("tm", None, "space", None, None),
        P("tm", None, "space", None, None),
        P("space", None, None),
        P("space", None, None),
        P("space", None, None),
        P(),
        P(),
    )
    out_specs = P("tm", None, "space", None, None)

    def body(*args):
        return local(*args, moves=moves)

    return jax.shard_map(body, mesh=mesh, in_specs=in_specs, out_specs=out_specs, check_vma=False)
```
